32 devices in a mesh: row: 8 (over z, y), col: 4 (over x, core).
Axes of the slice: x: 2, y: 2, z: 4, core: 2. Of those that a mesh axis runs over, the one named last changes fastest.
Arguments:
- eigvecs: float32 [131072, 1024], P('row', 'col'), may hold values from -6 to 6
- reflectors: float32 [4, 131072, 256], P(None, ('row', 'col'))
- factors: float32 [4, 256, 256], replicated, as said below
Outputs:
- transformed: float32 [131072, 1024], P('row', 'col')
The draws below stay inside these ranges and needn't reach their ends.
Inputs may be any that keep to these rules, and one draw needn't show every extreme that they name: Each factors[k] is upper triangular with a positive diagonal.
All inputs are finite; a program needn't handle non-finite values.
Results may differ from the reference program's by a relative error of at most 0.00012.
Values sent between devices are 32-bit elements; how exact they have to be, the bound alone decides.
A program may use at most 192 MiB of HBM per device.

```python
import jax
import jax.numpy as jnp
from jax import lax

N = 131072
M = 1024
WB = 256
PANELS = 4


def draw_reflectors(key, part):
    scale = (N * WB) ** (-0.25)
    base = jnp.clip(jax.random.normal(key, (PANELS, N, WB), jnp.float32), -6.0, 6.0)
    return base * scale


def draw_factors(key, part):
    diag = jax.random.uniform(key, (PANELS, WB), jnp.float32, 0.5, 1.5)
    off = 0.5 * jnp.clip(jax.random.normal(jax.random.fold_in(key, 3), (PANELS, WB, WB), jnp.float32), -6.0, 6.0) / jnp.sqrt(WB * 1.0)
    upper = jnp.triu(off, 1)
    eye = jnp.eye(WB, dtype=jnp.float32)
    return upper + eye[None, :, :] * diag[:, None, :]


def block_scale(rng, dims, pieces, low, top_value):
    def one(position, parts):
        heights = jax.random.uniform(jax.random.fold_in(jax.random.fold_in(rng, 6), position), (parts,), jnp.float32, low / len(pieces), top_value / len(pieces))
        return jnp.repeat(jnp.exp(heights), dims[position] // parts).reshape((-1,) + (1,) * (len(dims) - position - 1))

    factor_of = one(*pieces[0])
    for cut in pieces[1:]:
        factor_of = factor_of * one(*cut)
    return factor_of


def scatter_about(stream_key, dims, deviation, reach, split=(), kind=jnp.bfloat16):
    array = deviation * jax.random.normal(stream_key, dims, jnp.float32)
    if split:
        array = array * block_scale(stream_key, dims, split, -0.22, 0.18)
    return jnp.clip(array, -reach, reach).astype(kind)


def setup_inputs(seed: int = 0) -> dict:
    splits = jax.random.split(jax.random.key(seed), 4)
    return {
        "eigvecs": scatter_about(splits[0], (N, M), 1.0, 6.0, ((0, 8), (1, 4)), jnp.float32),
        "reflectors": draw_reflectors(jax.random.fold_in(splits[3], 71), 0),
        "factors": draw_factors(jax.random.fold_in(splits[3], 71), 0),
    }


def reference(eigvecs, reflectors, factors):
    field = eigvecs
    for index in range(PANELS):
        vectors = reflectors[index]
        proj = lax.dot_general(vectors, field, (((0,), (0,)), ((), ())), precision=lax.Precision.HIGHEST, preferred_element_type=jnp.float32)
        coeffs = jnp.dot(factors[index], proj, precision=lax.Precision.HIGHEST, preferred_element_type=jnp.float32)
        field = field - jnp.dot(vectors, coeffs, precision=lax.Precision.HIGHEST, preferred_element_type=jnp.float32)
    return field
```

```python
import functools

import jax
import jax.numpy as jnp
from jax import lax
from jax.experimental import pallas as pl
from jax.experimental.pallas import tpu as pltpu
from jax.sharding import PartitionSpec as P

CORES = 2
MESH = pl.DeviceIdType.MESH
SCOPED = 26 * 1024 * 1024


def tile_of(rows, most):
    tile = most
    while rows % tile:
        tile //= 2
    return tile


def halves(value):
    high = value.astype(jnp.bfloat16)
    low = (value - high.astype(jnp.float32)).astype(jnp.bfloat16)
    return high, low


def three_pass(left, right, dims):
    left_high, left_low = left
    right_high, right_low = right
    dot = functools.partial(lax.dot_general, dimension_numbers=(dims, ((), ())), preferred_element_type=jnp.float32)
    return dot(left_high, right_high) + (dot(left_high, right_low) + dot(left_low, right_high))


def fused_kernel(
    size, height, chunk,
    eig_ref, refl_ref, fac_ref,
    field_ref, last_ref, coeffs_ref,
    other_ref, acc_ref, proj_ref, pieces_ref, high_ref, low_ref,
    field_sem, own_sem, mate_send, mate_recv, far_send, far_recv, pass_send, pass_recv,
    credit, scatter_send, scatter_recv, gather_send, gather_recv,
):
    me = lax.axis_index("col")
    row = lax.axis_index("row")
    mate = me + 1 - 2 * (me % 2)
    shifts = list(range(CORES, size, CORES))
    panels, rows, width = refl_ref.shape
    chunks = rows // chunk
    piece = width // height
    tile = tile_of(rows, 512)

    def slot(k):
        return last_ref if (panels - 1 - k) % 2 == 0 else other_ref

    def block(owner, start, count):
        return pl.ds(pl.multiple_of(owner * rows + start, count), count)

    def own_copy(k):
        return pltpu.make_async_copy(refl_ref.at[k], slot(k).at[block(me, 0, rows)], own_sem.at[k % 2])

    def mate_copy(k, owner):
        return pltpu.make_async_remote_copy(
            src_ref=refl_ref.at[k], dst_ref=slot(k).at[block(owner, 0, rows)],
            send_sem=mate_send.at[k % 2], recv_sem=mate_recv.at[k % 2],
            device_id={"col": mate}, device_id_type=MESH)

    def far_copy(k, i, c, owner):
        return pltpu.make_async_remote_copy(
            src_ref=refl_ref.at[k, pl.ds(pl.multiple_of(c * chunk, chunk), chunk)],
            dst_ref=slot(k).at[block(owner, c * chunk, chunk)],
            send_sem=far_send.at[k % 2, i, c], recv_sem=far_recv.at[k % 2, i, c],
            device_id={"col": (me + shifts[i]) % size}, device_id_type=MESH)

    def pass_copy(k, i, c, owner):
        view = slot(k).at[block(owner, c * chunk, chunk)]
        return pltpu.make_async_remote_copy(
            src_ref=view, dst_ref=view,
            send_sem=pass_send.at[k % 2, i, c], recv_sem=pass_recv.at[k % 2, i, c],
            device_id={"col": mate}, device_id_type=MESH)

    def send(k):
        def one(c, carry):
            for i in range(len(shifts)):
                far_copy(k, i, c, me).start()
            return carry

        lax.fori_loop(0, chunks, one, 0)
        own_copy(k).start()
        mate_copy(k, me).start()

    def sent(k):
        def one(c, carry):
            for i in range(len(shifts)):
                far_copy(k, i, c, me).wait_send()
                pass_copy(k, i, c, (me - shifts[i] + size) % size).wait_send()
            return carry

        lax.fori_loop(0, chunks, one, 0)
        mate_copy(k, me).wait_send()

    def inner(k, owner, start, count):
        view = block(owner, start, count)
        acc_ref[...] += three_pass(halves(slot(k)[view, :]), halves(field_ref[view, :]), ((0,), (0,)))

    def inner_block(k, owner):
        def one(t, carry):
            inner(k, owner, t * tile, tile)
            return carry

        lax.fori_loop(0, rows // tile, one, 0)

    def reduce_row():
        def scatter(d):
            peer = (row + d) % height
            return pltpu.make_async_remote_copy(
                src_ref=acc_ref.at[pl.ds(pl.multiple_of(peer * piece, piece), piece)], dst_ref=pieces_ref.at[d],
                send_sem=scatter_send.at[d], recv_sem=scatter_recv.at[d],
                device_id={"row": peer}, device_id_type=MESH)

        def gather(d, owner):
            view = proj_ref.at[pl.ds(pl.multiple_of(owner * piece, piece), piece)]
            return pltpu.make_async_remote_copy(
                src_ref=view, dst_ref=view,
                send_sem=gather_send.at[d], recv_sem=gather_recv.at[d],
                device_id={"row": (row + d) % height}, device_id_type=MESH)

        mine = pl.ds(pl.multiple_of(row * piece, piece), piece)
        for d in range(1, height):
            scatter(d).start()
        total = acc_ref[mine, :]
        for d in range(1, height):
            scatter(d).wait_recv()
            total = total + pieces_ref[d]
        proj_ref[mine, :] = total
        for d in range(1, height):
            gather(d, row).start()
        for d in range(1, height):
            gather(d, (row - d + height) % height).wait_recv()
        for d in range(1, height):
            scatter(d).wait_send()
            gather(d, row).wait_send()

    barrier = pltpu.get_barrier_semaphore()
    for d in range(1, height):
        pl.semaphore_signal(barrier, inc=1, device_id={"row": (row + d) % height}, device_id_type=MESH)
    for there in [mate] + [(me + shift) % size for shift in shifts]:
        pl.semaphore_signal(barrier, inc=1, device_id={"col": there}, device_id_type=MESH)
    pl.semaphore_wait(barrier, height - 1 + 1 + len(shifts))

    field_copy = pltpu.make_async_copy(eig_ref, field_ref, field_sem)
    send(0)
    field_copy.start()
    if panels > 1:
        send(1)
    field_copy.wait()

    for k in range(panels):
        acc_ref[...] = jnp.zeros_like(acc_ref)
        own_copy(k).wait()
        inner_block(k, me)
        mate_copy(k, mate).wait_recv()
        inner_block(k, mate)

        def far_step(c, carry):
            for i in range(len(shifts)):
                owner = (me - shifts[i] + size) % size
                far_copy(k, i, c, owner).wait_recv()
                pass_copy(k, i, c, owner).start()
                inner(k, owner, c * chunk, chunk)
            for i in range(len(shifts)):
                owner = (mate - shifts[i] + size) % size
                pass_copy(k, i, c, owner).wait_recv()
                inner(k, owner, c * chunk, chunk)
            return carry

        lax.fori_loop(0, chunks, far_step, 0)
        reduce_row()
        coeffs = jnp.dot(fac_ref[k], proj_ref[...], precision=lax.Precision.HIGHEST, preferred_element_type=jnp.float32)
        if k == panels - 1:
            coeffs_ref[...] = coeffs
            break
        high_ref[...], low_ref[...] = halves(coeffs)

        def update_step(t, carry):
            view = pl.ds(pl.multiple_of(t * tile, tile), tile)
            field_ref[view, :] -= three_pass(halves(slot(k)[view, :]), (high_ref[...], low_ref[...]), ((1,), (0,)))
            return carry

        lax.fori_loop(0, size * rows // tile, update_step, 0)
        if k + 2 < panels:
            sent(k)
            for i in range(len(shifts)):
                pl.semaphore_signal(credit.at[k, i], inc=1, device_id={"col": (me - shifts[i] + size) % size}, device_id_type=MESH)
            pl.semaphore_signal(credit.at[k, len(shifts)], inc=1, device_id={"col": mate}, device_id_type=MESH)
            for i in range(len(shifts) + 1):
                pl.semaphore_wait(credit.at[k, i], 1)
            send(k + 2)
    for k in range(max(panels - 2, 0), panels):
        sent(k)


def fused(size, height, eigvecs, reflectors, factors):
    panels, rows, width = reflectors.shape
    total, columns = eigvecs.shape
    chunk = max(min(rows, 64), rows // 16)
    chunks = rows // chunk
    far = max(size // CORES - 1, 1)
    dma = pltpu.SemaphoreType.DMA
    return pl.pallas_call(
        functools.partial(fused_kernel, size, height, chunk),
        out_shape=[
            pltpu.VMEM((total, columns), jnp.float32),
            pltpu.VMEM((total, width), jnp.float32),
            pltpu.VMEM((width, columns), jnp.float32),
        ],
        in_specs=[pl.BlockSpec(memory_space=pl.ANY)] * 2 + [pl.BlockSpec(memory_space=pltpu.VMEM)],
        out_specs=[pl.BlockSpec(memory_space=pltpu.VMEM)] * 3,
        scratch_shapes=[
            pltpu.VMEM((total, width), jnp.float32),
            pltpu.VMEM((width, columns), jnp.float32),
            pltpu.VMEM((width, columns), jnp.float32),
            pltpu.VMEM((height, width // height, columns), jnp.float32),
            pltpu.VMEM((width, columns), jnp.bfloat16),
            pltpu.VMEM((width, columns), jnp.bfloat16),
            dma, dma((2,)), dma((2,)), dma((2,)),
            dma((2, far, chunks)), dma((2, far, chunks)), dma((2, far, chunks)), dma((2, far, chunks)),
            pltpu.SemaphoreType.REGULAR((max(panels, 1), far + 1)),
            dma((height,)), dma((height,)), dma((height,)), dma((height,)),
        ],
        compiler_params=pltpu.CompilerParams(collective_id=0, has_side_effects=True, vmem_limit_bytes=SCOPED),
        name="fused",
    )(*[pltpu.with_memory_space_constraint(value, pltpu.HBM) for value in (eigvecs, reflectors, factors)])


DEPTH = 4


def final_kernel(field_ref, vectors_ref, coeffs_ref, out_ref, high_ref, low_ref, stage_ref, sem):
    tile = stage_ref.shape[1]
    steps = field_ref.shape[0] // tile
    high_ref[...], low_ref[...] = halves(coeffs_ref[...])

    def store(t):
        view = pl.ds(pl.multiple_of(t * tile, tile), tile)
        return pltpu.make_async_copy(stage_ref.at[t % DEPTH], out_ref.at[view], sem.at[t % DEPTH])

    def step(t, carry):
        view = pl.ds(pl.multiple_of(t * tile, tile), tile)

        @pl.when(t >= DEPTH)
        def _():
            store(t - DEPTH).wait()

        stage_ref[t % DEPTH] = field_ref[view, :] - three_pass(halves(vectors_ref[view, :]), (high_ref[...], low_ref[...]), ((1,), (0,)))
        store(t).start()
        return carry

    lax.fori_loop(0, steps, step, 0)
    for t in range(max(steps - DEPTH, 0), steps):
        store(t).wait()


def final(field, vectors, coeffs):
    total, columns = field.shape
    width = vectors.shape[1]
    tile = tile_of(total, 512)
    return pl.pallas_call(
        final_kernel,
        out_shape=jax.ShapeDtypeStruct(field.shape, jnp.float32),
        in_specs=[pl.BlockSpec(memory_space=pltpu.VMEM)] * 3,
        out_specs=pl.BlockSpec(memory_space=pl.ANY),
        scratch_shapes=[
            pltpu.VMEM((width, columns), jnp.bfloat16),
            pltpu.VMEM((width, columns), jnp.bfloat16),
            pltpu.VMEM((DEPTH, tile, columns), jnp.float32),
            pltpu.SemaphoreType.DMA((DEPTH,)),
        ],
        compiler_params=pltpu.CompilerParams(vmem_limit_bytes=SCOPED),
        name="final",
    )(*[pltpu.with_memory_space_constraint(value, pltpu.VMEM) for value in (field, vectors, coeffs)])


def body(size, height, eigvecs, reflectors, factors):
    return final(*fused(size, height, eigvecs, reflectors, factors))


def solution(mesh):
    in_specs = (P("row", "col"), P(None, ("row", "col"), None), P())
    out_specs = P("row", "col")
    return jax.shard_map(functools.partial(body, mesh.shape["col"], mesh.shape["row"]), mesh=mesh, in_specs=in_specs, out_specs=out_specs, check_vma=False)
```

```python
import functools

import jax
import jax.numpy as jnp
from jax import lax
from jax.experimental import pallas as pl
from jax.experimental.pallas import tpu as pltpu
from jax.sharding import PartitionSpec as P

CORES = 2
MESH = pl.DeviceIdType.MESH
SCOPED = 26 * 1024 * 1024


def tile_of(rows, most):
    tile = most
    while rows % tile:
        tile //= 2
    return tile


def halves(value):
    high = value.astype(jnp.bfloat16)
    low = (value - high.astype(jnp.float32)).astype(jnp.bfloat16)
    return high, low


def three_pass(left, right, dims):
    left_high, left_low = left
    right_high, right_low = right
    left_dim, right_dim = dims
    left_all = jnp.concatenate([left_high, left_high, left_low], left_dim)
    right_all = jnp.concatenate([right_high, right_low, right_high], right_dim)
    return lax.dot_general(left_all, right_all, (((left_dim,), (right_dim,)), ((), ())), preferred_element_type=jnp.float32)


def whole_product(left, right):
    return jnp.dot(left, right, precision=lax.Precision.HIGHEST, preferred_element_type=jnp.float32)


def spans_of(width, height):
    half = width // 2
    return [(half, half), (0, half)] if half % 128 == 0 and half % (8 * height) == 0 else [(0, width)]


def fused_kernel(
    size, height, chunk,
    eig_ref, refl_ref, fac_ref,
    field_ref, last_ref, coeffs_ref,
    other_ref, acc_ref, proj_ref, pieces_ref, high_ref, low_ref, square_ref, rest_ref,
    field_sem, square_sem, token, own_sem, mate_send, mate_recv, far_send, far_recv, pass_send, pass_recv,
    credit, scatter_send, scatter_recv, gather_send, gather_recv,
):
    me = lax.axis_index("col")
    row = lax.axis_index("row")
    mate = me + 1 - 2 * (me % 2)
    shifts = list(range(CORES, size, CORES))
    panels, rows, width = refl_ref.shape
    chunks = rows // chunk
    tile = tile_of(rows, 1024)
    whole = (0, width)
    spans = spans_of(width, height)

    def slot(k):
        return last_ref if (panels - 1 - k) % 2 == 0 else other_ref

    def block(owner, start, count):
        return pl.ds(pl.multiple_of(owner * rows + start, count), count)

    def own_copy(k):
        return pltpu.make_async_copy(refl_ref.at[k], slot(k).at[block(me, 0, rows)], own_sem.at[k % 2])

    def mate_copy(k, owner):
        return pltpu.make_async_remote_copy(
            src_ref=refl_ref.at[k], dst_ref=slot(k).at[block(owner, 0, rows)],
            send_sem=mate_send.at[k % 2], recv_sem=mate_recv.at[k % 2],
            device_id={"col": mate}, device_id_type=MESH)

    def parts_of(k):
        if k < panels - 1 or len(spans) == 1:
            return [(k % 2, whole)]
        return [(k % 2, spans[0]), (2, spans[1])]

    def far_copy(k, part, i, c, owner):
        plane, (left, count) = part
        return pltpu.make_async_remote_copy(
            src_ref=refl_ref.at[k, pl.ds(pl.multiple_of(c * chunk, chunk), chunk), pl.ds(left, count)],
            dst_ref=slot(k).at[block(owner, c * chunk, chunk), pl.ds(left, count)],
            send_sem=far_send.at[plane, i, c], recv_sem=far_recv.at[plane, i, c],
            device_id={"col": (me + shifts[i]) % size}, device_id_type=MESH)

    def pass_copy(k, part, i, c, owner):
        plane, (left, count) = part
        view = slot(k).at[block(owner, c * chunk, chunk), pl.ds(left, count)]
        return pltpu.make_async_remote_copy(
            src_ref=view, dst_ref=view,
            send_sem=pass_send.at[plane, i, c], recv_sem=pass_recv.at[plane, i, c],
            device_id={"col": mate}, device_id_type=MESH)

    def send(k):
        for part in parts_of(k):
            def one(c, carry):
                for i in range(len(shifts)):
                    far_copy(k, part, i, c, me).start()
                return carry

            lax.fori_loop(0, chunks, one, 0)
        own_copy(k).start()
        mate_copy(k, me).start()

    def sent(k):
        for part in parts_of(k):
            def one(c, carry):
                for i in range(len(shifts)):
                    far_copy(k, part, i, c, me).wait_send()
                    pass_copy(k, part, i, c, (me - shifts[i] + size) % size).wait_send()
                return carry

            lax.fori_loop(0, chunks, one, 0)
        mate_copy(k, me).wait_send()

    def inner(k, span, owner, start, count):
        view = block(owner, start, count)
        left, many = span
        some = pl.ds(left, many)
        acc_ref[some, :] += three_pass(halves(slot(k)[view, some]), halves(field_ref[view, :]), (0, 0))

    def inner_block(k, owner):
        def one(t, carry):
            inner(k, whole, owner, t * tile, tile)
            return carry

        lax.fori_loop(0, rows // tile, one, 0)

    def far_chunk(k, part, c):
        for i in range(len(shifts)):
            owner = (me - shifts[i] + size) % size
            far_copy(k, part, i, c, owner).wait_recv()
            pass_copy(k, part, i, c, owner).start()
            inner(k, part[1], owner, c * chunk, chunk)
        for i in range(len(shifts)):
            owner = (mate - shifts[i] + size) % size
            pass_copy(k, part, i, c, owner).wait_recv()
            inner(k, part[1], owner, c * chunk, chunk)

    def update(k, span, view):
        some = pl.ds(*span)
        field_ref[view, :] -= three_pass(halves(slot(k)[view, some]), (high_ref[some, :], low_ref[some, :]), (1, 0))

    def reduce_row(span, between):
        first, many = span
        piece = many // height
        part = pl.ds(0, piece)

        def scatter(d):
            peer = (row + d) % height
            return pltpu.make_async_remote_copy(
                src_ref=acc_ref.at[pl.ds(pl.multiple_of(first + peer * piece, piece), piece)], dst_ref=pieces_ref.at[d, part],
                send_sem=scatter_send.at[d], recv_sem=scatter_recv.at[d],
                device_id={"row": peer}, device_id_type=MESH)

        def gather(d, owner):
            view = proj_ref.at[pl.ds(pl.multiple_of(first + owner * piece, piece), piece)]
            return pltpu.make_async_remote_copy(
                src_ref=view, dst_ref=view,
                send_sem=gather_send.at[d], recv_sem=gather_recv.at[d],
                device_id={"row": (row + d) % height}, device_id_type=MESH)

        mine = pl.ds(pl.multiple_of(first + row * piece, piece), piece)
        for d in range(1, height):
            scatter(d).start()
        between()
        total = acc_ref[mine, :]
        for d in range(1, height):
            scatter(d).wait_recv()
            total = total + pieces_ref[d, part, :]
        proj_ref[mine, :] = total
        for d in range(1, height):
            gather(d, row).start()
        for d in range(1, height):
            gather(d, (row - d + height) % height).wait_recv()
        for d in range(1, height):
            scatter(d).wait_send()
            gather(d, row).wait_send()

    barrier = pltpu.get_barrier_semaphore()
    for there in [mate] + [(me + shift) % size for shift in shifts]:
        pl.semaphore_signal(barrier, inc=1, device_id={"col": there}, device_id_type=MESH)
    lowest, highest = row == 0, row == height - 1
    below, above = jnp.maximum(row - 1, 0), jnp.minimum(row + 1, height - 1)

    @pl.when(jnp.logical_not(lowest))
    def _():
        pl.semaphore_signal(barrier, inc=1, device_id={"row": below}, device_id_type=MESH)

    @pl.when(jnp.logical_not(highest))
    def _():
        pl.semaphore_signal(barrier, inc=1, device_id={"row": above}, device_id_type=MESH)

    pl.semaphore_wait(barrier, 1 + len(shifts) + jnp.where(lowest, 0, 1) + jnp.where(highest, 0, 1))

    def greet_row():
        @pl.when(jnp.logical_not(lowest))
        def _():
            pl.semaphore_wait(token.at[0], 1)

        @pl.when(jnp.logical_not(highest))
        def _():
            pl.semaphore_signal(token.at[0], inc=1, device_id={"row": above}, device_id_type=MESH)
            pl.semaphore_wait(token.at[1], 1)

        @pl.when(jnp.logical_not(lowest))
        def _():
            pl.semaphore_signal(token.at[1], inc=1, device_id={"row": below}, device_id_type=MESH)

    field_copy = pltpu.make_async_copy(eig_ref, field_ref, field_sem)
    square_copy = pltpu.make_async_copy(fac_ref, square_ref, square_sem)
    send(0)
    field_copy.start()
    square_copy.start()
    if panels > 1:
        send(1)
    field_copy.wait()
    square_copy.wait()
    greet_row()

    def nothing():
        pass

    def finish():
        for k in range(max(panels - 2, 0), panels):
            sent(k)

    for k in range(panels):
        acc_ref[...] = jnp.zeros_like(acc_ref)
        own_copy(k).wait()
        inner_block(k, me)
        mate_copy(k, mate).wait_recv()
        inner_block(k, mate)
        first_part = parts_of(k)[0]

        def far_step(c, carry):
            far_chunk(k, first_part, c)
            return carry

        lax.fori_loop(0, chunks, far_step, 0)
        reduce_row(first_part[1], nothing)
        if k == panels - 1:
            break
        high_ref[...], low_ref[...] = halves(whole_product(square_ref[k], proj_ref[...]))

        def update_step(t, carry):
            update(k, whole, pl.ds(pl.multiple_of(t * tile, tile), tile))
            return carry

        lax.fori_loop(0, size * rows // tile, update_step, 0)
        if k + 2 < panels:
            sent(k)
            for i in range(len(shifts)):
                pl.semaphore_signal(credit.at[k, i], inc=1, device_id={"col": (me - shifts[i] + size) % size}, device_id_type=MESH)
            pl.semaphore_signal(credit.at[k, len(shifts)], inc=1, device_id={"col": mate}, device_id_type=MESH)
            for i in range(len(shifts) + 1):
                pl.semaphore_wait(credit.at[k, i], 1)
            send(k + 2)

    k = panels - 1
    if len(spans) == 1:
        finish()
        coeffs_ref[...] = whole_product(square_ref[k], proj_ref[...])
    else:
        (later, many), (_, few) = spans
        below, above = pl.ds(later, many), pl.ds(0, few)
        high_ref[below, :], low_ref[below, :] = halves(whole_product(square_ref[k, below, below], proj_ref[below, :]))
        rest_ref[...] = whole_product(square_ref[k, above, below], proj_ref[below, :])
        last_part = parts_of(k)[1]

        def update_far(c):
            for shift in shifts:
                for origin in (me, mate):
                    update(k, spans[0], block((origin - shift + size) % size, c * chunk, chunk))

        def last_step(c, carry):
            for origin in (me, mate):
                update(k, spans[0], block(origin, c * chunk, chunk))

            @pl.when(c > 0)
            def _():
                update_far(c - 1)

            far_chunk(k, last_part, c)
            return carry

        lax.fori_loop(0, chunks, last_step, 0)

        def meanwhile():
            update_far(chunks - 1)
            finish()

        reduce_row(spans[1], meanwhile)
        coeffs_ref[...] = rest_ref[...] + whole_product(square_ref[k, above, above], proj_ref[above, :])


def fused(size, height, eigvecs, reflectors, factors):
    panels, rows, width = reflectors.shape
    total, columns = eigvecs.shape
    chunk = max(min(rows, 64), rows // 16)
    chunks = rows // chunk
    kept = spans_of(width, height)[-1][1]
    far = max(size // CORES - 1, 1)
    dma = pltpu.SemaphoreType.DMA
    return pl.pallas_call(
        functools.partial(fused_kernel, size, height, chunk),
        out_shape=[
            pltpu.VMEM((total, columns), jnp.float32),
            pltpu.VMEM((total, width), jnp.float32),
            pltpu.VMEM((kept, columns), jnp.float32),
        ],
        in_specs=[pl.BlockSpec(memory_space=pl.ANY)] * 3,
        out_specs=[pl.BlockSpec(memory_space=pltpu.VMEM)] * 3,
        scratch_shapes=[
            pltpu.VMEM((total, width), jnp.float32),
            pltpu.VMEM((width, columns), jnp.float32),
            pltpu.VMEM((width, columns), jnp.float32),
            pltpu.VMEM((height, width // height, columns), jnp.float32),
            pltpu.VMEM((width, columns), jnp.bfloat16),
            pltpu.VMEM((width, columns), jnp.bfloat16),
            pltpu.VMEM((panels, width, width), jnp.float32),
            pltpu.VMEM((kept, columns), jnp.float32),
            dma, dma, pltpu.SemaphoreType.REGULAR((2,)), dma((2,)), dma((2,)), dma((2,)),
            dma((3, far, chunks)), dma((3, far, chunks)), dma((3, far, chunks)), dma((3, far, chunks)),
            pltpu.SemaphoreType.REGULAR((max(panels, 1), far + 1)),
            dma((height,)), dma((height,)), dma((height,)), dma((height,)),
        ],
        compiler_params=pltpu.CompilerParams(collective_id=0, has_side_effects=True, vmem_limit_bytes=SCOPED),
        name="fused",
    )(*[pltpu.with_memory_space_constraint(value, pltpu.HBM) for value in (eigvecs, reflectors, factors)])


DEPTH = 4


def final_kernel(field_ref, vectors_ref, coeffs_ref, out_ref, high_ref, low_ref, stage_ref, sem):
    tile = stage_ref.shape[1]
    steps = field_ref.shape[0] // tile
    kept = pl.ds(0, coeffs_ref.shape[0])
    high_ref[...], low_ref[...] = halves(coeffs_ref[...])

    def store(t):
        view = pl.ds(pl.multiple_of(t * tile, tile), tile)
        return pltpu.make_async_copy(stage_ref.at[t % DEPTH], out_ref.at[view], sem.at[t % DEPTH])

    def step(t, carry):
        view = pl.ds(pl.multiple_of(t * tile, tile), tile)

        @pl.when(t >= DEPTH)
        def _():
            store(t - DEPTH).wait()

        stage_ref[t % DEPTH] = field_ref[view, :] - three_pass(halves(vectors_ref[view, kept]), (high_ref[...], low_ref[...]), (1, 0))
        store(t).start()
        return carry

    lax.fori_loop(0, steps, step, 0)
    for t in range(max(steps - DEPTH, 0), steps):
        store(t).wait()


def final(field, vectors, coeffs):
    total, columns = field.shape
    width = coeffs.shape[0]
    tile = tile_of(total, 2048)
    return pl.pallas_call(
        final_kernel,
        out_shape=jax.ShapeDtypeStruct(field.shape, jnp.float32),
        in_specs=[pl.BlockSpec(memory_space=pltpu.VMEM)] * 3,
        out_specs=pl.BlockSpec(memory_space=pl.ANY),
        scratch_shapes=[
            pltpu.VMEM((width, columns), jnp.bfloat16),
            pltpu.VMEM((width, columns), jnp.bfloat16),
            pltpu.VMEM((DEPTH, tile, columns), jnp.float32),
            pltpu.SemaphoreType.DMA((DEPTH,)),
        ],
        compiler_params=pltpu.CompilerParams(vmem_limit_bytes=SCOPED),
        name="final",
    )(*[pltpu.with_memory_space_constraint(value, pltpu.VMEM) for value in (field, vectors, coeffs)])


def body(size, height, eigvecs, reflectors, factors):
    return final(*fused(size, height, eigvecs, reflectors, factors))


def solution(mesh):
    in_specs = (P("row", "col"), P(None, ("row", "col"), None), P())
    out_specs = P("row", "col")
    return jax.shard_map(functools.partial(body, mesh.shape["col"], mesh.shape["row"]), mesh=mesh, in_specs=in_specs, out_specs=out_specs, check_vma=False)
```

```python
import functools

import jax
import jax.numpy as jnp
from jax import lax
from jax.experimental import pallas as pl
from jax.experimental.pallas import tpu as pltpu
from jax.sharding import PartitionSpec as P

CORES = 2
MESH = pl.DeviceIdType.MESH
SCOPED = 26 * 1024 * 1024


def tile_of(rows, most):
    tile = most
    while rows % tile:
        tile //= 2
    return tile


def halves(value):
    high = value.astype(jnp.bfloat16)
    low = (value - high.astype(jnp.float32)).astype(jnp.bfloat16)
    return high, low


def three_pass(left, right, dims):
    left_high, left_low = left
    right_high, right_low = right
    left_dim, right_dim = dims
    left_all = jnp.concatenate([left_high, left_high, left_low], left_dim)
    right_all = jnp.concatenate([right_high, right_low, right_high], right_dim)
    return lax.dot_general(left_all, right_all, (((left_dim,), (right_dim,)), ((), ())), preferred_element_type=jnp.float32)


def whole_product(left, right):
    return jnp.dot(left, right, precision=lax.Precision.HIGHEST, preferred_element_type=jnp.float32)


def spans_of(width, height):
    half = width // 2
    return [(half, half), (0, half)] if half % 128 == 0 and half % (8 * height) == 0 else [(0, width)]


def fused_kernel(
    size, height, chunk,
    eig_ref, refl_ref, fac_ref,
    field_ref, last_ref, coeffs_ref,
    other_ref, acc_ref, proj_ref, pieces_ref, high_ref, low_ref, square_ref, rest_ref,
    field_sem, square_sem, token, own_sem, mate_send, mate_recv, far_send, far_recv, pass_send, pass_recv,
    credit, scatter_send, scatter_recv, gather_send, gather_recv,
):
    me = lax.axis_index("col")
    row = lax.axis_index("row")
    mate = me + 1 - 2 * (me % 2)
    shifts = list(range(CORES, size, CORES))
    panels, rows, width = refl_ref.shape
    chunks = rows // chunk
    tile = tile_of(rows, 1024)
    whole = (0, width)
    spans = spans_of(width, height)

    def slot(k):
        return last_ref if (panels - 1 - k) % 2 == 0 else other_ref

    def block(owner, start, count):
        return pl.ds(pl.multiple_of(owner * rows + start, count), count)

    def own_copy(k):
        return pltpu.make_async_copy(refl_ref.at[k], slot(k).at[block(me, 0, rows)], own_sem.at[k % 2])

    def mate_copy(k, owner):
        return pltpu.make_async_remote_copy(
            src_ref=refl_ref.at[k], dst_ref=slot(k).at[block(owner, 0, rows)],
            send_sem=mate_send.at[k % 2], recv_sem=mate_recv.at[k % 2],
            device_id={"col": mate}, device_id_type=MESH)

    def parts_of(k):
        if k < panels - 1 or len(spans) == 1:
            return [(k % 2, whole)]
        return [(k % 2, spans[0]), (2, spans[1])]

    def far_copy(k, part, i, c, owner):
        plane, (left, count) = part
        return pltpu.make_async_remote_copy(
            src_ref=refl_ref.at[k, pl.ds(pl.multiple_of(c * chunk, chunk), chunk), pl.ds(left, count)],
            dst_ref=slot(k).at[block(owner, c * chunk, chunk), pl.ds(left, count)],
            send_sem=far_send.at[plane, i, c], recv_sem=far_recv.at[plane, i, c],
            device_id={"col": (me + shifts[i]) % size}, device_id_type=MESH)

    def pass_copy(k, part, i, c, owner):
        plane, (left, count) = part
        view = slot(k).at[block(owner, c * chunk, chunk), pl.ds(left, count)]
        return pltpu.make_async_remote_copy(
            src_ref=view, dst_ref=view,
            send_sem=pass_send.at[plane, i, c], recv_sem=pass_recv.at[plane, i, c],
            device_id={"col": mate}, device_id_type=MESH)

    def send(k):
        for part in parts_of(k):
            def one(c, carry):
                for i in range(len(shifts)):
                    far_copy(k, part, i, c, me).start()
                return carry

            lax.fori_loop(0, chunks, one, 0)
        own_copy(k).start()
        mate_copy(k, me).start()

    def sent(k):
        for part in parts_of(k):
            def one(c, carry):
                for i in range(len(shifts)):
                    far_copy(k, part, i, c, me).wait_send()
                    pass_copy(k, part, i, c, (me - shifts[i] + size) % size).wait_send()
                return carry

            lax.fori_loop(0, chunks, one, 0)
        mate_copy(k, me).wait_send()

    def inner(k, span, owner, start, count):
        view = block(owner, start, count)
        left, many = span
        some = pl.ds(left, many)
        acc_ref[some, :] += three_pass(halves(slot(k)[view, some]), halves(field_ref[view, :]), (0, 0))

    def inner_block(k, owner):
        def one(t, carry):
            inner(k, whole, owner, t * tile, tile)
            return carry

        lax.fori_loop(0, rows // tile, one, 0)

    def near_chunk(k, part, c):
        for i in range(len(shifts)):
            owner = (me - shifts[i] + size) % size
            far_copy(k, part, i, c, owner).wait_recv()
            pass_copy(k, part, i, c, owner).start()
            inner(k, part[1], owner, c * chunk, chunk)

    def passed_chunk(k, part, c):
        for i in range(len(shifts)):
            owner = (mate - shifts[i] + size) % size
            pass_copy(k, part, i, c, owner).wait_recv()
            inner(k, part[1], owner, c * chunk, chunk)

    def update(k, span, view):
        some = pl.ds(*span)
        field_ref[view, :] -= three_pass(halves(slot(k)[view, some]), (high_ref[some, :], low_ref[some, :]), (1, 0))

    def reduce_row(span, between):
        first, many = span
        piece = many // height
        part = pl.ds(0, piece)

        def scatter(d):
            peer = (row + d) % height
            return pltpu.make_async_remote_copy(
                src_ref=acc_ref.at[pl.ds(pl.multiple_of(first + peer * piece, piece), piece)], dst_ref=pieces_ref.at[d, part],
                send_sem=scatter_send.at[d], recv_sem=scatter_recv.at[d],
                device_id={"row": peer}, device_id_type=MESH)

        def gather(d, owner):
            view = proj_ref.at[pl.ds(pl.multiple_of(first + owner * piece, piece), piece)]
            return pltpu.make_async_remote_copy(
                src_ref=view, dst_ref=view,
                send_sem=gather_send.at[d], recv_sem=gather_recv.at[d],
                device_id={"row": (row + d) % height}, device_id_type=MESH)

        mine = pl.ds(pl.multiple_of(first + row * piece, piece), piece)
        for d in range(1, height):
            scatter(d).start()
        between()
        total = acc_ref[mine, :]
        for d in range(1, height):
            scatter(d).wait_recv()
            total = total + pieces_ref[d, part, :]
        proj_ref[mine, :] = total
        for d in range(1, height):
            gather(d, row).start()
        for d in range(1, height):
            gather(d, (row - d + height) % height).wait_recv()
        for d in range(1, height):
            scatter(d).wait_send()
            gather(d, row).wait_send()

    barrier = pltpu.get_barrier_semaphore()
    for there in [mate] + [(me + shift) % size for shift in shifts]:
        pl.semaphore_signal(barrier, inc=1, device_id={"col": there}, device_id_type=MESH)
    lowest, highest = row == 0, row == height - 1
    below, above = jnp.maximum(row - 1, 0), jnp.minimum(row + 1, height - 1)

    @pl.when(jnp.logical_not(lowest))
    def _():
        pl.semaphore_signal(barrier, inc=1, device_id={"row": below}, device_id_type=MESH)

    @pl.when(jnp.logical_not(highest))
    def _():
        pl.semaphore_signal(barrier, inc=1, device_id={"row": above}, device_id_type=MESH)

    pl.semaphore_wait(barrier, 1 + len(shifts) + jnp.where(lowest, 0, 1) + jnp.where(highest, 0, 1))

    def greet_row():
        @pl.when(jnp.logical_not(lowest))
        def _():
            pl.semaphore_wait(token.at[0], 1)

        @pl.when(jnp.logical_not(highest))
        def _():
            pl.semaphore_signal(token.at[0], inc=1, device_id={"row": above}, device_id_type=MESH)
            pl.semaphore_wait(token.at[1], 1)

        @pl.when(jnp.logical_not(lowest))
        def _():
            pl.semaphore_signal(token.at[1], inc=1, device_id={"row": below}, device_id_type=MESH)

    field_copy = pltpu.make_async_copy(eig_ref, field_ref, field_sem)
    square_copy = pltpu.make_async_copy(fac_ref, square_ref, square_sem)
    send(0)
    field_copy.start()
    square_copy.start()
    if panels > 1:
        send(1)
    field_copy.wait()
    square_copy.wait()
    greet_row()

    def nothing():
        pass

    def finish():
        for k in range(max(panels - 2, 0), panels):
            sent(k)

    for k in range(panels):
        acc_ref[...] = jnp.zeros_like(acc_ref)
        own_copy(k).wait()
        inner_block(k, me)
        mate_copy(k, mate).wait_recv()
        inner_block(k, mate)
        first_part = parts_of(k)[0]

        def far_step(c, carry):
            near_chunk(k, first_part, c)

            @pl.when(c > 0)
            def _():
                passed_chunk(k, first_part, c - 1)

            return carry

        lax.fori_loop(0, chunks, far_step, 0)
        passed_chunk(k, first_part, chunks - 1)
        reduce_row(first_part[1], nothing)
        if k == panels - 1:
            break
        high_ref[...], low_ref[...] = halves(whole_product(square_ref[k], proj_ref[...]))

        def update_step(t, carry):
            update(k, whole, pl.ds(pl.multiple_of(t * tile, tile), tile))
            return carry

        lax.fori_loop(0, size * rows // tile, update_step, 0)
        if k + 2 < panels:
            sent(k)
            for i in range(len(shifts)):
                pl.semaphore_signal(credit.at[k, i], inc=1, device_id={"col": (me - shifts[i] + size) % size}, device_id_type=MESH)
            pl.semaphore_signal(credit.at[k, len(shifts)], inc=1, device_id={"col": mate}, device_id_type=MESH)
            for i in range(len(shifts) + 1):
                pl.semaphore_wait(credit.at[k, i], 1)
            send(k + 2)

    k = panels - 1
    if len(spans) == 1:
        finish()
        coeffs_ref[...] = whole_product(square_ref[k], proj_ref[...])
    else:
        (later, many), (_, few) = spans
        below, above = pl.ds(later, many), pl.ds(0, few)
        high_ref[below, :], low_ref[below, :] = halves(whole_product(square_ref[k, below, below], proj_ref[below, :]))
        rest_ref[...] = whole_product(square_ref[k, above, below], proj_ref[below, :])
        last_part = parts_of(k)[1]

        def update_far(c):
            for shift in shifts:
                for origin in (me, mate):
                    update(k, spans[0], block((origin - shift + size) % size, c * chunk, chunk))

        def last_step(c, carry):
            for origin in (me, mate):
                update(k, spans[0], block(origin, c * chunk, chunk))

            @pl.when(c > 1)
            def _():
                update_far(c - 2)

            near_chunk(k, last_part, c)

            @pl.when(c > 0)
            def _():
                passed_chunk(k, last_part, c - 1)

            return carry

        lax.fori_loop(0, chunks, last_step, 0)
        passed_chunk(k, last_part, chunks - 1)

        def meanwhile():
            for c in range(max(chunks - 2, 0), chunks):
                update_far(c)
            finish()

        reduce_row(spans[1], meanwhile)
        coeffs_ref[...] = rest_ref[...] + whole_product(square_ref[k, above, above], proj_ref[above, :])


def fused(size, height, eigvecs, reflectors, factors):
    panels, rows, width = reflectors.shape
    total, columns = eigvecs.shape
    chunk = max(min(rows, 64), rows // 16)
    chunks = rows // chunk
    kept = spans_of(width, height)[-1][1]
    far = max(size // CORES - 1, 1)
    dma = pltpu.SemaphoreType.DMA
    return pl.pallas_call(
        functools.partial(fused_kernel, size, height, chunk),
        out_shape=[
            pltpu.VMEM((total, columns), jnp.float32),
            pltpu.VMEM((total, width), jnp.float32),
            pltpu.VMEM((kept, columns), jnp.float32),
        ],
        in_specs=[pl.BlockSpec(memory_space=pl.ANY)] * 3,
        out_specs=[pl.BlockSpec(memory_space=pltpu.VMEM)] * 3,
        scratch_shapes=[
            pltpu.VMEM((total, width), jnp.float32),
            pltpu.VMEM((width, columns), jnp.float32),
            pltpu.VMEM((width, columns), jnp.float32),
            pltpu.VMEM((height, width // height, columns), jnp.float32),
            pltpu.VMEM((width, columns), jnp.bfloat16),
            pltpu.VMEM((width, columns), jnp.bfloat16),
            pltpu.VMEM((panels, width, width), jnp.float32),
            pltpu.VMEM((kept, columns), jnp.float32),
            dma, dma, pltpu.SemaphoreType.REGULAR((2,)), dma((2,)), dma((2,)), dma((2,)),
            dma((3, far, chunks)), dma((3, far, chunks)), dma((3, far, chunks)), dma((3, far, chunks)),
            pltpu.SemaphoreType.REGULAR((max(panels, 1), far + 1)),
            dma((height,)), dma((height,)), dma((height,)), dma((height,)),
        ],
        compiler_params=pltpu.CompilerParams(collective_id=0, has_side_effects=True, vmem_limit_bytes=SCOPED),
        name="fused",
    )(*[pltpu.with_memory_space_constraint(value, pltpu.HBM) for value in (eigvecs, reflectors, factors)])


DEPTH = 4


def final_kernel(field_ref, vectors_ref, coeffs_ref, out_ref, high_ref, low_ref, stage_ref, sem):
    tile = stage_ref.shape[1]
    steps = field_ref.shape[0] // tile
    kept = pl.ds(0, coeffs_ref.shape[0])
    high_ref[...], low_ref[...] = halves(coeffs_ref[...])

    def store(t):
        view = pl.ds(pl.multiple_of(t * tile, tile), tile)
        return pltpu.make_async_copy(stage_ref.at[t % DEPTH], out_ref.at[view], sem.at[t % DEPTH])

    def step(t, carry):
        view = pl.ds(pl.multiple_of(t * tile, tile), tile)

        @pl.when(t >= DEPTH)
        def _():
            store(t - DEPTH).wait()

        stage_ref[t % DEPTH] = field_ref[view, :] - three_pass(halves(vectors_ref[view, kept]), (high_ref[...], low_ref[...]), (1, 0))
        store(t).start()
        return carry

    lax.fori_loop(0, steps, step, 0)
    for t in range(max(steps - DEPTH, 0), steps):
        store(t).wait()


def final(field, vectors, coeffs):
    total, columns = field.shape
    width = coeffs.shape[0]
    tile = tile_of(total, 2048)
    return pl.pallas_call(
        final_kernel,
        out_shape=jax.ShapeDtypeStruct(field.shape, jnp.float32),
        in_specs=[pl.BlockSpec(memory_space=pltpu.VMEM)] * 3,
        out_specs=pl.BlockSpec(memory_space=pl.ANY),
        scratch_shapes=[
            pltpu.VMEM((width, columns), jnp.bfloat16),
            pltpu.VMEM((width, columns), jnp.bfloat16),
            pltpu.VMEM((DEPTH, tile, columns), jnp.float32),
            pltpu.SemaphoreType.DMA((DEPTH,)),
        ],
        compiler_params=pltpu.CompilerParams(vmem_limit_bytes=SCOPED),
        name="final",
    )(*[pltpu.with_memory_space_constraint(value, pltpu.VMEM) for value in (field, vectors, coeffs)])


def body(size, height, eigvecs, reflectors, factors):
    return final(*fused(size, height, eigvecs, reflectors, factors))


def solution(mesh):
    in_specs = (P("row", "col"), P(None, ("row", "col"), None), P())
    out_specs = P("row", "col")
    return jax.shard_map(functools.partial(body, mesh.shape["col"], mesh.shape["row"]), mesh=mesh, in_specs=in_specs, out_specs=out_specs, check_vma=False)
```
